32 devices in a mesh: freq: 8 (over z, y), pts: 4 (over x, core).
Axes of the slice: x: 2, y: 2, z: 4, core: 2. Of those that a mesh axis runs over, the one named last changes fastest.
Arguments:
- direct: bfloat16 [8, 512, 6144], P('freq', None, 'pts'), may hold values from -6 to 6
- onsets: int32 [8, 6144], P('freq', 'pts'), may hold values from 64 to 511
- left_bases: bfloat16 [128, 24, 24, 2, 8, 256], P('freq', 'pts'), may hold values from -0.4375 to 0.4375
- right_bases: bfloat16 [128, 24, 24, 2, 8, 256], P('freq', 'pts'), may hold values from -0.25 to 0.25
- tile_ranks: int32 [128, 24, 24], P('freq', 'pts'), may hold values from 1 to 8
Outputs:
- plus_field: float32 [8, 512, 6144], P('freq', None, 'pts')
- minus_field: float32 [8, 512, 6144], P('freq', None, 'pts')
The draws below stay inside these ranges and needn't reach their ends.
All inputs are finite; a program needn't handle non-finite values.
Results may differ from the reference program's by a relative error of at most 0.017.
Values may be sent and summed in bfloat16 or wider, within the bound.
No kernel may reach another device: no remote copies, remote signals or barrier semaphores. Data moves between devices by JAX's collectives and lax.ppermute only.
A program may use at most 256 MiB of HBM per device.

```python
import math
import jax
import jax.numpy as jnp
from jax import lax

N = 6144
NB = 256
K = 8
F = 128
ITERS = 3
NT = 512
NTL = 24
P_SIZE = 8
N_PTS = 4


def place_ends(drawn, own_key, least, top_value):
    longest = drawn.shape.index(max(drawn.shape))
    spots = []
    for shift in (0, 1):
        where = [jax.random.randint(jax.random.fold_in(own_key, axis), (), 0, length) for axis, length in enumerate(drawn.shape)]
        where[longest] = (where[longest] + shift) % drawn.shape[longest]
        spots.append(tuple(where))
    return drawn.at[spots[0]].set(least).at[spots[1]].set(top_value)


def block_scale(stream_key, shape, shards, smallest, top_value):
    level = 1.0
    for position, parts in shards:
        steps = jax.random.uniform(jax.random.fold_in(jax.random.fold_in(stream_key, 6), position), (parts,), jnp.float32, smallest / len(shards), top_value / len(shards))
        level = level * jnp.repeat(jnp.exp(steps), shape[position] // parts).reshape((-1,) + (1,) * (len(shape) - 1 - position))
    return level


def gaussian(rng, dims, spread, most, cuts=(), dtype=jnp.bfloat16):
    array = spread * jax.random.normal(rng, dims, jnp.float32)
    if cuts:
        array = array * block_scale(rng, dims, cuts, -0.22, 0.18)
    return jnp.clip(array, -most, most).astype(dtype)


def setup_inputs(seed: int = 0) -> dict:
    seeds = jax.random.split(jax.random.key(seed), 6)
    return {
        "direct": gaussian(seeds[0], (P_SIZE, NT, N), 1.0, 6.0, ((0, 8), (2, 4))),
        "onsets": place_ends(jax.random.randint(seeds[1], (P_SIZE, N), NT // 8, NT), jax.random.fold_in(seeds[1], 1), NT // 8, NT - 1).astype(jnp.int32),
        "left_bases": gaussian(seeds[2], (F, NTL, NTL, 2, K, NB), (N // NB * K) ** -0.5, 0.4375, ((0, 8), (1, 4))),
        "right_bases": gaussian(seeds[3], (F, NTL, NTL, 2, K, NB), (2 * NB) ** -0.5, 0.25, ((0, 8), (1, 4))),
        "tile_ranks": place_ends(jax.random.randint(seeds[4], (F, NTL, NTL), 1, K + 1), jax.random.fold_in(seeds[4], 1), 1, K).astype(jnp.int32),
    }


HIGHEST = lax.Precision.HIGHEST

def band_tables(freq_total, sample_total):
    bins = lax.broadcasted_iota(jnp.int32, (freq_total, sample_total), 0) + 1
    moments = lax.broadcasted_iota(jnp.int32, (freq_total, sample_total), 1)
    phases = 2.0 * math.pi / sample_total * (bins * moments % sample_total).astype(jnp.float32)
    scaling = 1.0 / math.sqrt(sample_total)
    cosine = jnp.cos(phases) * scaling
    sine = jnp.sin(phases) * scaling
    return (jnp.stack([cosine, -sine]), jnp.stack([2.0 * cosine, -2.0 * sine]))

def rounded(values):
    return lax.optimization_barrier(values.astype(jnp.bfloat16)).astype(jnp.float32)

def contract(spec, left_part, right_part):
    return jnp.einsum(spec, left_part.astype(jnp.float32), right_part.astype(jnp.float32), precision=HIGHEST)

def conj_apply(spec, basis_real, basis_imag, vector_real, vector_imag):
    real_part = contract(spec, basis_real, vector_real) + contract(spec, basis_imag, vector_imag)
    imag_part = contract(spec, basis_real, vector_imag) - contract(spec, basis_imag, vector_real)
    return (real_part, imag_part)

def plain_apply(spec, basis_real, basis_imag, vector_real, vector_imag):
    real_part = contract(spec, basis_real, vector_real) - contract(spec, basis_imag, vector_imag)
    imag_part = contract(spec, basis_real, vector_imag) + contract(spec, basis_imag, vector_real)
    return (real_part, imag_part)

def reference(direct, onsets, left_bases, right_bases, tile_ranks):
    forward_exact, inverse_exact = band_tables(F, NT)
    forward_table = rounded(forward_exact)
    inverse_table = rounded(inverse_exact)
    point_total = direct.shape[0]
    tile_count = N // NB
    tile_group = tile_count // N_PTS
    moments = lax.broadcasted_iota(jnp.int32, direct.shape, 1)
    window = (moments < onsets[:, None, :]).astype(jnp.float32)
    rank_index = lax.broadcasted_iota(jnp.int32, tile_ranks.shape + (K,), 3)
    rank_mask = (rank_index < tile_ranks[..., None]).astype(jnp.float32)[..., None]

    def to_band(history):
        samples = rounded(history)
        spectrum = jnp.einsum('cft,ptn->cfpn', forward_table, samples, precision=HIGHEST)
        spectrum = spectrum.reshape(2, F, point_total, tile_count, NB).astype(jnp.bfloat16)
        return jnp.moveaxis(spectrum, 1, 0)

    def to_time(spectrum):
        flat = jnp.moveaxis(spectrum, 0, 1).reshape(2, F, point_total, N).astype(jnp.float32)
        return jnp.einsum('cft,cfpn->ptn', inverse_table, flat, precision=HIGHEST) * window

    def forward_one(operands):
        spectrum, left_part, right_part, mask_part = operands
        real_part, imag_part = conj_apply('ijkb,pjb->ijkp', right_part[:, :, 0], right_part[:, :, 1], spectrum[0], spectrum[1])
        terms = (jnp.stack([real_part, imag_part]) * mask_part).astype(jnp.bfloat16)
        real_part, imag_part = plain_apply('ijkb,ijkp->pib', left_part[:, :, 0], left_part[:, :, 1], terms[0], terms[1])
        return jnp.stack([real_part, imag_part]).astype(jnp.bfloat16)

    def adjoint_one(operands):
        spectrum, left_part, right_part, mask_part = operands
        real_part, imag_part = conj_apply('ijkb,pib->ijkp', left_part[:, :, 0], left_part[:, :, 1], spectrum[0], spectrum[1])
        terms = (jnp.stack([real_part, imag_part]) * mask_part).astype(jnp.bfloat16)
        terms = terms.reshape(2, N_PTS, tile_group, tile_count, K, point_total)
        grouped = right_part.reshape(N_PTS, tile_group, tile_count, 2, K, NB)
        real_part, imag_part = plain_apply('gijkb,gijkp->gpjb', grouped[:, :, :, 0], grouped[:, :, :, 1], terms[0], terms[1])
        partial_value = jnp.stack([real_part, imag_part], axis=1).astype(jnp.bfloat16)
        partial_value = lax.optimization_barrier(partial_value).astype(jnp.float32)
        return lax.optimization_barrier(jnp.sum(partial_value, axis=0)).astype(jnp.bfloat16)
    history = direct.astype(jnp.float32)
    plus_field = history
    minus_field = jnp.zeros_like(history)
    for iteration in range(ITERS):
        spectra = lax.map(forward_one, (to_band(history), left_bases, right_bases, rank_mask))
        reflected = to_time(spectra)
        minus_field = minus_field + reflected
        spectra = lax.map(adjoint_one, (to_band(reflected), left_bases, right_bases, rank_mask))
        history = to_time(spectra)
        plus_field = plus_field + history
    return (plus_field, minus_field)
```

```python
import functools
import math

import jax
import jax.numpy as jnp
from jax import lax
from jax.experimental import pallas as pl
from jax.experimental.pallas import tpu as pltpu
from jax.sharding import PartitionSpec as P

ITERS = 3
LANES = 128


def band_tables(freq_total, sample_total):
    bins = lax.broadcasted_iota(jnp.int32, (freq_total, sample_total), 0) + 1
    moments = lax.broadcasted_iota(jnp.int32, (freq_total, sample_total), 1)
    phases = 2.0 * math.pi / sample_total * (bins * moments % sample_total).astype(jnp.float32)
    scaling = 1.0 / math.sqrt(sample_total)
    cosine = jnp.cos(phases) * scaling
    sine = jnp.sin(phases) * scaling
    return (jnp.stack([cosine, -sine]), jnp.stack([2.0 * cosine, -2.0 * sine]))


def coefficients(basis, field, pair):
    wide = field.astype(jnp.float32)
    half = wide.shape[0] // 2
    turned = jnp.concatenate([wide[half:], -wide[:half]], axis=0)
    both = jnp.concatenate([wide, turned], axis=0).astype(jnp.bfloat16)
    products = lax.dot_general(
        basis, both, (((1,), (1,)), ((), ())), preferred_element_type=jnp.float32
    )
    width = 2 * half
    direct = products[:, :width].reshape(-1, 2, pair, width)
    other = products[:, width:].reshape(-1, 2, pair, width)
    real_rows = direct[:, 0] + other[:, 1]
    imag_rows = direct[:, 1] - other[:, 0]
    return jnp.stack([real_rows, imag_rows], axis=1)


def spread(coeffs, mask_row):
    return (jnp.transpose(coeffs) * mask_row).astype(jnp.bfloat16)


def forward_kernel(x_ref, left_ref, right_ref, mask_ref, y_ref, scratch, *, rank):
    tile_rows, tile_columns, pair, nb = left_ref.shape[1:]
    width = x_ref.shape[2]
    per_group = x_ref.shape[3] // nb
    for column in range(tile_columns):
        group, place = divmod(column, per_group)
        field = x_ref[group, 0, :, place * nb : (place + 1) * nb]
        basis = right_ref[0, :, column].reshape(tile_rows * pair, nb)
        terms = coefficients(basis, field, rank)
        scratch[:, column * pair : (column + 1) * pair, :width] = terms.reshape(
            tile_rows, pair, width
        )
    for row in range(tile_rows):
        weights = spread(scratch[row], mask_ref[0, row : row + 1, :])[:width]
        basis = left_ref[0, row].reshape(tile_columns * pair, nb)
        value = jnp.dot(weights, basis, preferred_element_type=jnp.float32)
        y_ref[0, :, row * nb : (row + 1) * nb] = value.astype(jnp.bfloat16)


def adjoint_kernel(y_ref, left_ref, right_ref, mask_ref, z_ref, scratch, *, rank):
    tile_rows, tile_columns, pair, nb = left_ref.shape[1:]
    width = y_ref.shape[1]
    per_group = z_ref.shape[3] // nb
    used = tile_rows * pair
    for row in range(tile_rows):
        field = y_ref[0, :, row * nb : (row + 1) * nb]
        basis = left_ref[0, row].reshape(tile_columns * pair, nb)
        terms = coefficients(basis, field, rank)
        scratch[:, row * pair : (row + 1) * pair, :width] = terms.reshape(
            tile_columns, pair, width
        )
    for column in range(tile_columns):
        group, place = divmod(column, per_group)
        weights = spread(scratch[column], mask_ref[0, column : column + 1, :])[:width, :used]
        basis = right_ref[0, :, column].reshape(used, nb)
        value = jnp.dot(weights, basis, preferred_element_type=jnp.float32)
        z_ref[group, 0, :, place * nb : (place + 1) * nb] = value.astype(jnp.bfloat16)


def round_up(value, step):
    return -(-value // step) * step


def body(direct, onsets, left_bases, right_bases, tile_ranks):
    point_here, sample_total, cells_here = direct.shape
    freq_here, tile_rows, tile_columns, _, rank, nb = left_bases.shape
    freq_size = lax.axis_size("freq")
    pts_size = lax.axis_size("pts")
    freq_total = freq_here * freq_size
    point_total = point_here * freq_size
    width = 2 * point_total
    pair = 2 * rank
    forward_exact, inverse_exact = band_tables(freq_total, sample_total)
    forward_table = jnp.swapaxes(forward_exact, 0, 1).reshape(2 * freq_total, sample_total)
    forward_table = forward_table.astype(jnp.bfloat16)
    inverse_table = jnp.swapaxes(inverse_exact, 0, 1).reshape(2 * freq_total, sample_total)
    inverse_table = inverse_table.T.astype(jnp.bfloat16)

    moments = lax.broadcasted_iota(jnp.int32, direct.shape, 1)
    window = moments < onsets[:, None, :]

    rank_index = lax.broadcasted_iota(jnp.int32, tile_ranks.shape + (2, rank), 4)
    mask = (rank_index < tile_ranks[..., None, None]).astype(jnp.float32)
    mask = mask.reshape(freq_here, tile_rows, tile_columns, pair)
    forward_mask = mask.reshape(freq_here, tile_rows, tile_columns * pair)
    used = tile_rows * pair
    padded = round_up(used, LANES)
    adjoint_mask = jnp.swapaxes(mask, 1, 2).reshape(freq_here, tile_columns, used)
    adjoint_mask = jnp.pad(adjoint_mask, ((0, 0), (0, 0), (0, padded - used)))

    left = left_bases.reshape(freq_here, tile_rows, tile_columns, pair, nb)
    right = right_bases.reshape(freq_here, tile_rows, tile_columns, pair, nb)

    rows = freq_here * width
    to_row = lax.broadcasted_iota(jnp.int32, (rows, rows), 0)
    from_row = lax.broadcasted_iota(jnp.int32, (rows, rows), 1)
    source = (to_row % point_total) * (2 * freq_here) + to_row // point_total
    gather_rows = (source == from_row).astype(jnp.bfloat16)
    scatter_rows = gather_rows.T

    params = pltpu.CompilerParams(
        dimension_semantics=("arbitrary",), vmem_limit_bytes=48 * 1024 * 1024
    )
    basis_spec = pl.BlockSpec((1, tile_rows, tile_columns, pair, nb), lambda f: (f, 0, 0, 0, 0))
    own_spec = pl.BlockSpec((1, width, cells_here), lambda f: (f, 0, 0))
    all_spec = pl.BlockSpec((pts_size, 1, width, cells_here), lambda f: (0, f, 0, 0))
    lane_width = round_up(width, LANES)
    forward_tiles = pl.pallas_call(
        functools.partial(forward_kernel, rank=rank),
        grid=(freq_here,),
        in_specs=[
            all_spec,
            basis_spec,
            basis_spec,
            pl.BlockSpec((1, tile_rows, tile_columns * pair), lambda f: (f, 0, 0)),
        ],
        out_specs=own_spec,
        out_shape=jax.ShapeDtypeStruct((freq_here, width, cells_here), jnp.bfloat16),
        scratch_shapes=[pltpu.VMEM((tile_rows, tile_columns * pair, lane_width), jnp.float32)],
        compiler_params=params,
        name="forward_tiles",
    )
    adjoint_tiles = pl.pallas_call(
        functools.partial(adjoint_kernel, rank=rank),
        grid=(freq_here,),
        in_specs=[
            own_spec,
            basis_spec,
            basis_spec,
            pl.BlockSpec((1, tile_columns, padded), lambda f: (f, 0, 0)),
        ],
        out_specs=all_spec,
        out_shape=jax.ShapeDtypeStruct((pts_size, freq_here, width, cells_here), jnp.bfloat16),
        scratch_shapes=[pltpu.VMEM((tile_columns, padded, lane_width), jnp.float32)],
        compiler_params=params,
        name="adjoint_tiles",
    )

    def to_band(history):
        samples = history.astype(jnp.bfloat16)
        spectrum = jnp.einsum(
            "gt,ptn->pgn", forward_table, samples, preferred_element_type=jnp.float32
        ).astype(jnp.bfloat16)
        spectrum = spectrum.reshape(point_here, freq_size, 2 * freq_here, cells_here)
        spectrum = jnp.swapaxes(spectrum, 0, 1)
        arrived = lax.all_to_all(spectrum, "freq", split_axis=0, concat_axis=0, tiled=True)
        arrived = arrived.reshape(rows, cells_here)
        ordered = jnp.dot(gather_rows, arrived, preferred_element_type=jnp.float32)
        return ordered.astype(jnp.bfloat16).reshape(freq_here, width, cells_here)

    def to_time(ordered):
        ordered = ordered.reshape(freq_size, point_here, 2 * freq_here, cells_here)
        arrived = lax.all_to_all(ordered, "freq", split_axis=0, concat_axis=0, tiled=True)
        flat = jnp.swapaxes(arrived, 0, 1).reshape(point_here, 2 * freq_total, cells_here)
        field = jnp.einsum(
            "tg,pgn->ptn", inverse_table, flat, preferred_element_type=jnp.float32
        )
        return jnp.where(window, field, 0.0)

    def forward_apply(spectrum):
        everywhere = lax.all_gather(spectrum, "pts", axis=0, tiled=False)
        value = forward_tiles(everywhere, left, right, forward_mask)
        value = jnp.dot(
            scatter_rows, value.reshape(rows, cells_here), preferred_element_type=jnp.float32
        )
        return value.astype(jnp.bfloat16)

    def adjoint_apply(spectrum):
        partial_value = adjoint_tiles(spectrum, left, right, adjoint_mask)
        arrived = lax.all_to_all(partial_value, "pts", split_axis=0, concat_axis=0, tiled=True)
        arrived = arrived.reshape(pts_size, rows, cells_here)
        value = jnp.einsum(
            "rs,gsn->rn", scatter_rows, arrived, preferred_element_type=jnp.float32
        )
        return value.astype(jnp.bfloat16)

    plus_field = direct.astype(jnp.float32)
    minus_field = jnp.zeros_like(plus_field)
    history = direct
    for _ in range(ITERS):
        reflected = to_time(forward_apply(to_band(history)))
        minus_field = minus_field + reflected
        history = to_time(adjoint_apply(to_band(reflected)))
        plus_field = plus_field + history
    return (plus_field, minus_field)


def solution(mesh):
    return jax.shard_map(
        body,
        mesh=mesh,
        in_specs=(
            P("freq", None, "pts"),
            P("freq", "pts"),
            P("freq", "pts", None, None, None, None),
            P("freq", "pts", None, None, None, None),
            P("freq", "pts", None),
        ),
        out_specs=(P("freq", None, "pts"), P("freq", None, "pts")),
        check_vma=False,
    )
```

```python
import functools
import math

import jax
import jax.numpy as jnp
from jax import lax
from jax.experimental import pallas as pl
from jax.experimental.pallas import tpu as pltpu
from jax.sharding import PartitionSpec as P

ITERS = 3
CHUNKS = 2
LANES = 128


def band_tables(freq_total, sample_total):
    bins = lax.broadcasted_iota(jnp.int32, (freq_total, sample_total), 0) + 1
    moments = lax.broadcasted_iota(jnp.int32, (freq_total, sample_total), 1)
    phases = 2.0 * math.pi / sample_total * (bins * moments % sample_total).astype(jnp.float32)
    scaling = 1.0 / math.sqrt(sample_total)
    cosine = jnp.cos(phases) * scaling
    sine = jnp.sin(phases) * scaling
    return (jnp.stack([cosine, -sine]), jnp.stack([2.0 * cosine, -2.0 * sine]))


def coefficients(basis, field, pair):
    wide = field.astype(jnp.float32)
    half = wide.shape[0] // 2
    turned = jnp.concatenate([wide[half:], -wide[:half]], axis=0)
    both = jnp.concatenate([wide, turned], axis=0).astype(jnp.bfloat16)
    products = lax.dot_general(
        basis, both, (((1,), (1,)), ((), ())), preferred_element_type=jnp.float32
    )
    width = 2 * half
    direct = products[:, :width].reshape(-1, 2, pair, width)
    other = products[:, width:].reshape(-1, 2, pair, width)
    real_rows = direct[:, 0] + other[:, 1]
    imag_rows = direct[:, 1] - other[:, 0]
    return jnp.stack([real_rows, imag_rows], axis=1)


def spread(coeffs, mask_row):
    return (jnp.transpose(coeffs) * mask_row).astype(jnp.bfloat16)


def forward_kernel(x_ref, left_ref, right_ref, mask_ref, y_ref, scratch, *, rank):
    tile_rows, tile_columns, pair, nb = left_ref.shape[1:]
    width = x_ref.shape[2]
    per_group = x_ref.shape[3] // nb
    for column in range(tile_columns):
        group, place = divmod(column, per_group)
        field = x_ref[group, 0, :, place * nb : (place + 1) * nb]
        basis = right_ref[0, :, column].reshape(tile_rows * pair, nb)
        terms = coefficients(basis, field, rank)
        scratch[:, column * pair : (column + 1) * pair, :width] = terms.reshape(
            tile_rows, pair, width
        )
    for row in range(tile_rows):
        weights = spread(scratch[row], mask_ref[0, row : row + 1, :])[:width]
        basis = left_ref[0, row].reshape(tile_columns * pair, nb)
        value = jnp.dot(weights, basis, preferred_element_type=jnp.float32)
        y_ref[0, :, row * nb : (row + 1) * nb] = value.astype(jnp.bfloat16)


def adjoint_kernel(y_ref, left_ref, right_ref, mask_ref, z_ref, scratch, *, rank):
    tile_rows, tile_columns, pair, nb = left_ref.shape[1:]
    width = y_ref.shape[1]
    per_group = z_ref.shape[3] // nb
    used = tile_rows * pair
    for row in range(tile_rows):
        field = y_ref[0, :, row * nb : (row + 1) * nb]
        basis = left_ref[0, row].reshape(tile_columns * pair, nb)
        terms = coefficients(basis, field, rank)
        scratch[:, row * pair : (row + 1) * pair, :width] = terms.reshape(
            tile_columns, pair, width
        )
    for column in range(tile_columns):
        group, place = divmod(column, per_group)
        weights = spread(scratch[column], mask_ref[0, column : column + 1, :])[:width, :used]
        basis = right_ref[0, :, column].reshape(used, nb)
        value = jnp.dot(weights, basis, preferred_element_type=jnp.float32)
        z_ref[group, 0, :, place * nb : (place + 1) * nb] = value.astype(jnp.bfloat16)


def round_up(value, step):
    return -(-value // step) * step


def body(direct, onsets, left_bases, right_bases, tile_ranks):
    point_here, sample_total, cells_here = direct.shape
    freq_here, tile_rows, tile_columns, _, rank, nb = left_bases.shape
    freq_size = lax.axis_size("freq")
    pts_size = lax.axis_size("pts")
    freq_total = freq_here * freq_size
    point_total = point_here * freq_size
    width = 2 * point_total
    pair = 2 * rank
    forward_exact, inverse_exact = band_tables(freq_total, sample_total)
    chunks = CHUNKS if freq_here % CHUNKS == 0 else 1
    freq_chunk = freq_here // chunks

    def chunk_rows(table, chunk):
        rows = jnp.swapaxes(table, 0, 1).reshape(freq_size, chunks, 2 * freq_chunk, sample_total)
        return rows[:, chunk].reshape(-1, sample_total).astype(jnp.bfloat16)

    forward_tables = [chunk_rows(forward_exact, chunk) for chunk in range(chunks)]
    inverse_tables = [chunk_rows(inverse_exact, chunk).T for chunk in range(chunks)]

    moments = lax.broadcasted_iota(jnp.int32, direct.shape, 1)
    window = moments < onsets[:, None, :]

    rank_index = lax.broadcasted_iota(jnp.int32, tile_ranks.shape + (2, rank), 4)
    mask = (rank_index < tile_ranks[..., None, None]).astype(jnp.float32)
    mask = mask.reshape(freq_here, tile_rows, tile_columns, pair)
    forward_mask = mask.reshape(freq_here, tile_rows, tile_columns * pair)
    used = tile_rows * pair
    padded = round_up(used, LANES)
    adjoint_mask = jnp.swapaxes(mask, 1, 2).reshape(freq_here, tile_columns, used)
    adjoint_mask = jnp.pad(adjoint_mask, ((0, 0), (0, 0), (0, padded - used)))

    left = left_bases.reshape(freq_here, tile_rows, tile_columns, pair, nb)
    right = right_bases.reshape(freq_here, tile_rows, tile_columns, pair, nb)

    rows = freq_chunk * width
    to_row = lax.broadcasted_iota(jnp.int32, (rows, rows), 0)
    from_row = lax.broadcasted_iota(jnp.int32, (rows, rows), 1)
    source = (to_row % point_total) * (2 * freq_chunk) + to_row // point_total
    gather_rows = (source == from_row).astype(jnp.bfloat16)
    scatter_rows = gather_rows.T
    gather_rows, scatter_rows = lax.optimization_barrier((gather_rows, scatter_rows))

    params = pltpu.CompilerParams(
        dimension_semantics=("arbitrary",), vmem_limit_bytes=48 * 1024 * 1024
    )
    own_spec = pl.BlockSpec((1, width, cells_here), lambda f: (f, 0, 0))
    all_spec = pl.BlockSpec((pts_size, 1, width, cells_here), lambda f: (0, f, 0, 0))
    own_shape = jax.ShapeDtypeStruct((freq_chunk, width, cells_here), jnp.bfloat16)
    all_shape = jax.ShapeDtypeStruct((pts_size, freq_chunk, width, cells_here), jnp.bfloat16)
    lane_width = round_up(width, LANES)
    flops = 2 * freq_chunk * tile_rows * tile_columns * pair * nb * 3 * width
    cost = pl.CostEstimate(
        flops=flops * 16,
        transcendentals=0,
        bytes_accessed=freq_chunk * tile_rows * tile_columns * pair * nb * 4,
    )

    def tiles(kernel, chunk, in_spec, out_spec, out_shape, mask_shape, scratch, name):
        first = chunk * freq_chunk
        basis_spec = pl.BlockSpec(
            (1, tile_rows, tile_columns, pair, nb), lambda f: (f + first, 0, 0, 0, 0)
        )
        return pl.pallas_call(
            functools.partial(kernel, rank=rank),
            grid=(freq_chunk,),
            in_specs=[
                in_spec,
                basis_spec,
                basis_spec,
                pl.BlockSpec((1,) + mask_shape, lambda f: (f + first, 0, 0)),
            ],
            out_specs=out_spec,
            out_shape=out_shape,
            scratch_shapes=[pltpu.VMEM(scratch, jnp.float32)],
            compiler_params=params,
            cost_estimate=cost,
            name=name,
        )

    def forward_tiles(spectrum, chunk):
        call = tiles(
            forward_kernel, chunk, all_spec, own_spec, own_shape,
            (tile_rows, tile_columns * pair),
            (tile_rows, tile_columns * pair, lane_width), "forward_tiles",
        )
        return call(spectrum, left, right, forward_mask)

    def adjoint_tiles(spectrum, chunk):
        call = tiles(
            adjoint_kernel, chunk, own_spec, all_spec, all_shape,
            (tile_columns, padded), (tile_columns, padded, lane_width), "adjoint_tiles",
        )
        return call(spectrum, left, right, adjoint_mask)

    def to_band(samples, chunk):
        spectrum = jnp.einsum(
            "gt,ptn->pgn", forward_tables[chunk], samples, preferred_element_type=jnp.float32
        ).astype(jnp.bfloat16)
        spectrum = spectrum.reshape(point_here, freq_size, 2 * freq_chunk, cells_here)
        spectrum = jnp.swapaxes(spectrum, 0, 1)
        arrived = lax.all_to_all(spectrum, "freq", split_axis=0, concat_axis=0, tiled=True)
        arrived = arrived.reshape(rows, cells_here)
        ordered = jnp.dot(gather_rows, arrived, preferred_element_type=jnp.float32)
        return ordered.astype(jnp.bfloat16).reshape(freq_chunk, width, cells_here)

    def to_time(ordered_chunks):
        field = 0.0
        for chunk, ordered in enumerate(ordered_chunks):
            ordered = ordered.reshape(freq_size, point_here, 2 * freq_chunk, cells_here)
            arrived = lax.all_to_all(ordered, "freq", split_axis=0, concat_axis=0, tiled=True)
            flat = jnp.swapaxes(arrived, 0, 1).reshape(point_here, -1, cells_here)
            field = field + jnp.einsum(
                "tg,pgn->ptn", inverse_tables[chunk], flat, preferred_element_type=jnp.float32
            )
        return jnp.where(window, field, 0.0)

    def forward_apply(spectrum, chunk):
        everywhere = lax.all_gather(spectrum, "pts", axis=0, tiled=False)
        value = forward_tiles(everywhere, chunk)
        value = jnp.dot(
            scatter_rows, value.reshape(rows, cells_here), preferred_element_type=jnp.float32
        )
        return value.astype(jnp.bfloat16)

    def adjoint_apply(spectrum, chunk):
        partial_value = adjoint_tiles(spectrum, chunk)
        value = lax.psum_scatter(partial_value, "pts", scatter_dimension=0, tiled=False)
        value = value.reshape(rows, cells_here)
        value = jnp.dot(scatter_rows, value, preferred_element_type=jnp.float32)
        return value.astype(jnp.bfloat16)

    def turn(field, apply):
        samples = field.astype(jnp.bfloat16)
        spectra = [to_band(samples, chunk) for chunk in range(chunks)]
        return to_time([apply(spectrum, chunk) for chunk, spectrum in enumerate(spectra)])

    plus_field = direct.astype(jnp.float32)
    minus_field = jnp.zeros_like(plus_field)
    history = direct
    for _ in range(ITERS):
        reflected = turn(history, forward_apply)
        minus_field = minus_field + reflected
        history = turn(reflected, adjoint_apply)
        plus_field = plus_field + history
    return (plus_field, minus_field)


def solution(mesh):
    return jax.shard_map(
        body,
        mesh=mesh,
        in_specs=(
            P("freq", None, "pts"),
            P("freq", "pts"),
            P("freq", "pts", None, None, None, None),
            P("freq", "pts", None, None, None, None),
            P("freq", "pts", None),
        ),
        out_specs=(P("freq", None, "pts"), P("freq", None, "pts")),
        check_vma=False,
    )
```
